32 devices in a mesh: dp: 4 (over x, y), ep: 8 (over z, core).
Axes of the slice: x: 2, y: 2, z: 4, core: 2. Of those that a mesh axis runs over, the one named last changes fastest.
Arguments:
- x: bfloat16 [4, 8, 256, 4096], P('dp', 'ep'), parts along dimension 0
- expert: int32 [4, 8, 256, 2], P('dp', 'ep'), parts along dimension 0
- slot: int32 [4, 8, 256, 2], P('dp', 'ep'), parts along dimension 0
- gate: float32 [4, 8, 256, 2], P('dp', 'ep'), parts along dimension 0
- w_gate: bfloat16 [16, 4096, 6400], P('ep')
- w_up: bfloat16 [16, 4096, 6400], P('ep')
- w_down: bfloat16 [16, 6400, 4096], P('ep')
Outputs:
- y: bfloat16 [4, 8, 256, 4096], P('dp', 'ep'), parts along dimension 0
There are 4 independent parts. The reference program is written for one: setup_inputs(seed, part) draws one part's arguments, and reference() takes and returns one part's arrays. A program takes and returns all parts, laid end to end along the dimension named above; an argument that names none is the same for every part.
All inputs are finite; a program needn't handle non-finite values.
Results may differ from the reference program's by a relative error of at most 0.009.
Values are sent between devices in bfloat16 or wider.
A program may use at most 2 GiB of HBM per device.

```python
import jax
import jax.numpy as jnp

MEMBERS = 8
TOKENS = 256
D = 4096
FF = 6400
TOP = 2
EXPERTS = 16
SLOTS = 5 * TOKENS * TOP // (4 * EXPERTS)


def setup_inputs(seed: int = 0, part: int = 0) -> dict:
    own, k1, k2, k3, k4, k5, k6 = jax.random.split(jax.random.key(seed), 7)
    kx, ke, kl, kg = jax.random.split(jax.random.fold_in(own, part), 4)
    devices = (1, MEMBERS)
    place = jax.random.permutation(kl, jnp.arange(EXPERTS, dtype=jnp.uint32))
    slow = ((EXPERTS + (9 * place) % EXPERTS) << ((9 * place) // EXPERTS)) // EXPERTS
    wait = (jax.random.bits(ke, (*devices, TOKENS, EXPERTS), jnp.uint32) >> 10) * slow
    expert = jnp.argsort(wait, axis=-1)[..., :TOP].astype(jnp.int32)
    chosen = jax.nn.one_hot(expert, EXPERTS, dtype=jnp.int32)
    in_line = jnp.cumsum(chosen.reshape(*devices, TOKENS * TOP, EXPERTS), axis=2) - 1
    slot = jnp.sum(in_line.reshape(chosen.shape) * chosen, axis=-1)

    def one(key, rows, columns):
        return (jax.random.normal(key, (rows, columns), jnp.float32) * rows**-0.5).astype(jnp.bfloat16)

    def weights(key, rows, columns):
        return jax.lax.map(lambda k: one(k, rows, columns), jax.random.split(key, EXPERTS))

    return {
        "x": jax.random.normal(kx, (*devices, TOKENS, D), jnp.float32).astype(jnp.bfloat16),
        "expert": expert,
        "slot": slot,
        "gate": jax.nn.softmax(jax.random.normal(kg, expert.shape, jnp.float32)),
        "w_gate": weights(k1, D, FF),
        "w_up": weights(k2, D, FF),
        "w_down": weights(k3, FF, D),
    }


def einsum(form, a, b):
    return jnp.einsum(form, a.astype(jnp.float32), b.astype(jnp.float32))


def reference(x, expert, slot, gate, w_gate, w_up, w_down):
    to_expert = jax.nn.one_hot(expert, EXPERTS, dtype=jnp.bfloat16)
    to_slot = jax.nn.one_hot(slot, SLOTS, dtype=jnp.bfloat16)
    weighted = to_expert * gate[..., None].astype(jnp.bfloat16)
    dispatch = einsum("abtke,abtkc->abtec", to_expert, to_slot).astype(jnp.bfloat16)
    combine = einsum("abtke,abtkc->abtec", weighted, to_slot).astype(jnp.bfloat16)
    z = einsum("abtec,abtd->aebcd", dispatch, x).astype(jnp.bfloat16)
    h = jax.nn.silu(einsum("aebcd,edf->aebcf", z, w_gate))
    h = (h * einsum("aebcd,edf->aebcf", z, w_up)).astype(jnp.bfloat16)
    out = einsum("aebcf,efd->aebcd", h, w_down).astype(jnp.bfloat16)
    y = einsum("abtec,aebcd->abtd", combine, out)
    return y.astype(jnp.bfloat16)
```

```python
import functools

import jax
import jax.numpy as jnp
from jax import lax
from jax.experimental import pallas as pl
from jax.experimental.pallas import tpu as pltpu
from jax.sharding import PartitionSpec as P

TILE = 256
STEPS_IN, STEPS_OUT = 5, 4


def ffn_kernel(z_hbm, w_gate, w_up, w_down, o_hbm, pool, z, h, stage, sem, z_sem, o_sem, *, k):
    rows, d = z.shape
    ff = h.shape[1]
    wide, deep = ff // STEPS_IN, d // STEPS_OUT

    def load_in(t, slot):
        c = pl.ds(pl.multiple_of(t * wide, 128), wide)
        return [
            pltpu.make_async_copy(w_gate.at[k, :, c], pool.at[slot, pl.ds(0, d), :], sem.at[slot, 0]),
            pltpu.make_async_copy(w_up.at[k, :, c], pool.at[slot, pl.ds(d, d), :], sem.at[slot, 1]),
        ]

    def load_first(i):
        c = pl.ds(i * TILE, TILE)
        return [
            pltpu.make_async_copy(w_gate.at[k, :, c], pool.at[0, pl.ds(0, d), c], sem.at[0, 2 * i]),
            pltpu.make_async_copy(w_up.at[k, :, c], pool.at[0, pl.ds(d, d), c], sem.at[0, 2 * i + 1]),
        ]

    def load_out(t, slot):
        c = pl.ds(pl.multiple_of(t * deep, 128), deep)
        return pltpu.make_async_copy(w_down.at[k, :, c], pool.at[slot, pl.ds(0, ff), pl.ds(0, deep)], sem.at[slot, 0])

    def store(t, slot):
        c = pl.ds(pl.multiple_of(t * deep, 128), deep)
        return pltpu.make_async_copy(stage.at[slot], o_hbm.at[:, c], o_sem.at[slot])

    def project_in(t, slot, i):
        c = pl.ds(i * TILE, TILE)
        g = jnp.dot(z[...], pool[slot, pl.ds(0, d), c], preferred_element_type=jnp.float32)
        u = jnp.dot(z[...], pool[slot, pl.ds(d, d), c], preferred_element_type=jnp.float32)
        h[:, pl.ds(pl.multiple_of(t * wide + i * TILE, 128), TILE)] = (g * jax.nn.sigmoid(g) * u).astype(h.dtype)

    tokens = pltpu.make_async_copy(z_hbm, z, z_sem)
    for i in range(wide // TILE):
        for copy in load_first(i):
            copy.start()
        if i == 0:
            tokens.start()

    for i in range(wide // TILE):
        for copy in load_first(i):
            copy.wait()
        if i == 0:
            tokens.wait()
            for copy in load_in(1, 1):
                copy.start()
        project_in(0, 0, i)

    @pl.loop(1, STEPS_IN)
    def _(t):
        slot = lax.rem(t, 2)
        for copy in load_in(t, slot):
            copy.wait()

        @pl.when(t + 1 < STEPS_IN)
        def _():
            for copy in load_in(t + 1, 1 - slot):
                copy.start()

        @pl.when(t + 1 == STEPS_IN)
        def _():
            load_out(0, 1 - slot).start()

        for i in range(wide // TILE):
            project_in(t, slot, i)

    @pl.loop(0, STEPS_OUT)
    def _(t):
        slot, mine = lax.rem(t + STEPS_IN, 2), lax.rem(t, 2)
        load_out(t, slot).wait()

        @pl.when(t + 1 < STEPS_OUT)
        def _():
            load_out(t + 1, 1 - slot).start()

        @pl.when(t >= 2)
        def _():
            store(t - 2, mine).wait()

        for i in range(deep // TILE):
            c = pl.ds(i * TILE, TILE)
            out = jnp.dot(h[...], pool[slot, pl.ds(0, ff), c], preferred_element_type=jnp.float32)
            stage[mine, :, c] = out.astype(stage.dtype)
        store(t, mine).start()

    for t in range(STEPS_OUT - 2, STEPS_OUT):
        store(t, t % 2).wait()


def ffn(z, w_gate, w_up, w_down, k):
    (rows, d), ff = z.shape, w_gate.shape[2]
    anywhere = pl.BlockSpec(memory_space=pl.ANY)
    return pl.pallas_call(
        functools.partial(ffn_kernel, k=k),
        in_specs=[anywhere] * 4,
        out_specs=anywhere,
        out_shape=jax.ShapeDtypeStruct((rows, d), jnp.bfloat16),
        scratch_shapes=[
            pltpu.VMEM((2, 2 * d, ff // STEPS_IN), jnp.bfloat16),
            pltpu.VMEM((rows, d), jnp.bfloat16),
            pltpu.VMEM((rows, ff), jnp.bfloat16),
            pltpu.VMEM((2, rows, d // STEPS_OUT), jnp.bfloat16),
            pltpu.SemaphoreType.DMA((2, 2 * ff // STEPS_IN // TILE)),
            pltpu.SemaphoreType.DMA,
            pltpu.SemaphoreType.DMA((2,)),
        ],
        compiler_params=pltpu.CompilerParams(vmem_limit_bytes=60 * 2**20),
        cost_estimate=pl.CostEstimate(flops=6 * rows * d * ff, bytes_accessed=6 * d * ff, transcendentals=0),
        name=f"ffn{k}",
    )(z, w_gate, w_up, w_down)


def solution(mesh):
    devices = mesh.shape["ep"]

    def body(x, expert, slot, gate, w_gate, w_up, w_down):
        x, expert, slot, gate = x[0, 0], expert[0, 0], slot[0, 0], gate[0, 0]
        (tokens, d), top = x.shape, expert.shape[1]
        local = w_gate.shape[0]
        experts = devices * local
        slots = 5 * tokens * top // (4 * experts)
        place = jnp.where(slot < slots, expert * slots + slot, -1)
        weight = gate.astype(jnp.bfloat16)

        def rows_of(k):
            e = jnp.arange(devices, dtype=jnp.int32)[:, None] * local + k
            return (e * slots + jnp.arange(slots, dtype=jnp.int32)).reshape(-1)

        zs = []
        for k in range(local):
            dispatch = jnp.any(rows_of(k)[:, None, None] == place[None], axis=2).astype(jnp.bfloat16)
            sent = jnp.dot(dispatch, x, preferred_element_type=jnp.float32).astype(jnp.bfloat16)
            z = lax.all_to_all(sent.reshape(devices, slots, d), "ep", 0, 0)
            zs.append(z.reshape(devices * slots, d))
        y = 0
        for k in range(local):
            out = ffn(zs[k], w_gate, w_up, w_down, k)
            back = lax.all_to_all(out.reshape(devices, slots, d), "ep", 0, 0)
            hit = rows_of(k)[None, :, None] == place[:, None]
            combine = jnp.sum(jnp.where(hit, weight[:, None], 0), axis=2, dtype=jnp.bfloat16)
            y += jnp.dot(combine, back.reshape(devices * slots, d), preferred_element_type=jnp.float32)
        return y.astype(jnp.bfloat16)[None, None]

    by_token, by_expert = P("dp", "ep", None, None), P("ep", None, None)
    return jax.shard_map(
        body,
        mesh=mesh,
        in_specs=(by_token,) * 4 + (by_expert,) * 3,
        out_specs=by_token,
        check_vma=False,
    )
```
